256 devices in a mesh: row: 16 (over y, z_hi), col: 16 (over x, z_lo, core).
Axes of the slice: x: 4, y: 4, z: 8 (z_hi: 4, z_lo: 2; z = z_hi * 2 + z_lo), core: 2. Of those that a mesh axis runs over, the one named last changes fastest.
Arguments:
- left_act: bfloat16 [1536, 128], P(('row', 'col')), may hold values from -540 to 540
- right_act: bfloat16 [1536, 128], P(('row', 'col')), may hold values from -6 to 6
- norm_gain: float32 [128], replicated, may hold values from 0.25 to 1.75
- norm_bias: float32 [128], replicated, may hold values from -3 to 3
- w_in: bfloat16 [128, 512], replicated, may hold values from -0.5 to 0.5
- b_in: float32 [512], replicated, may hold values from -3 to 3
- w_out: bfloat16 [512, 128], replicated, may hold values from -0.25 to 0.25
- w_bins: bfloat16 [128, 64], replicated, may hold values from -0.5 to 0.5
- labels: int32 [1536, 1536], P('row', 'col'), may hold values from 0 to 63, as said below
Outputs:
- grad_left: float32 [1536, 128], P(('row', 'col'))
- grad_right: float32 [1536, 128], P('col')
- grad_w_in: float32 [128, 512], replicated
- grad_w_out: float32 [512, 128], replicated
- grad_w_bins: float32 [128, 64], replicated
The draws below stay inside these ranges and needn't reach their ends.
Inputs may be any that keep to these rules, and one draw needn't show every extreme that they name: labels is symmetric: labels[i, j] equals labels[j, i].
All inputs are finite; a program needn't handle non-finite values.
Results may differ from the reference program's by a relative error of at most 0.00039.
Values may be sent and summed in bfloat16 or wider, within the bound.
No kernel may reach another device: no remote copies, remote signals or barrier semaphores. Data moves between devices by JAX's collectives and lax.ppermute only.
A program may use at most 64 MiB of HBM per device.

```python
import jax
import jax.numpy as jnp
from jax import lax

C = 128
H = 512
BINS = 64
L = 1536


def draw_left_act(key, part):
    sample = jnp.clip(jax.random.normal(key, (L, C), jnp.float32), -6.0, 6.0)
    return sample.astype(jnp.bfloat16)


def draw_labels(key, part):
    upper = jax.random.randint(key, (L, L), 0, BINS)
    places = lax.iota(jnp.int32, L)
    upper_half = places[:, None] <= places[None, :]
    return jnp.where(upper_half, upper, upper.T)


def shard_levels(stream_key, dims, shards, low, top_value):
    def one(dim, blocks):
        draws = jax.random.uniform(jax.random.fold_in(jax.random.fold_in(stream_key, 6), dim), (blocks,), jnp.float32, low / len(shards), top_value / len(shards))
        return jnp.repeat(jnp.exp(draws), dims[dim] // blocks).reshape((-1,) + (1,) * (len(dims) - dim - 1))

    factor_of = one(*shards[0])
    for cut in shards[1:]:
        factor_of = factor_of * one(*cut)
    return factor_of


def scatter_about(stream_key, dims, scale, bound, cuts=(), held_as=jnp.bfloat16):
    level = shard_levels(stream_key, dims, cuts, -0.22, 0.18) if cuts else 1.0
    entries = jax.random.normal(stream_key, dims, jnp.float32) * scale * level
    return jnp.minimum(jnp.maximum(entries, -bound), bound).astype(held_as)


def setup_inputs(seed: int = 0) -> dict:
    seeds = jax.random.split(jax.random.key(seed), 10)
    left_act = draw_left_act(jax.random.fold_in(seeds[9], 71), 0)
    right_act = scatter_about(seeds[1], (L, C), 1.0, 6.0, ((0, 256),))
    norm_gain = jnp.clip(1.0 + 0.15 * jax.random.normal(seeds[2], (C,), jnp.float32), 0.25, 1.75)
    norm_bias = scatter_about(seeds[3], (C,), 0.5, 3.0, (), jnp.float32)
    w_in = scatter_about(seeds[4], (C, H), C ** -0.5, 0.5)
    b_in = scatter_about(seeds[5], (H,), 0.5, 3.0, (), jnp.float32)
    w_out = scatter_about(seeds[6], (H, C), H ** -0.5, 0.25)
    w_bins = scatter_about(seeds[7], (C, BINS), C ** -0.5, 0.5)
    labels = draw_labels(jax.random.fold_in(seeds[9], 71), 0)
    return {"left_act": left_act, "right_act": right_act, "norm_gain": norm_gain, "norm_bias": norm_bias, "w_in": w_in, "b_in": b_in, "w_out": w_out, "w_bins": w_bins, "labels": labels}


def inner(first, second):
    return lax.dot_general(first, second, (((0,), (0,)), ((), ())), preferred_element_type=jnp.float32)

def outer(first, second):
    return lax.dot_general(first, second, (((1,), (1,)), ((), ())), preferred_element_type=jnp.float32)

def transition(left_rows, right_cols, gain, bias, w_in, b_in, w_out):
    summed = (left_rows.astype(jnp.float32)[:, None, :] + right_cols.astype(jnp.float32)[None, :, :]).reshape(-1, left_rows.shape[1])
    center = summed - lax.optimization_barrier(jnp.mean(summed, axis=-1, keepdims=True))
    inv_scale = lax.rsqrt(lax.optimization_barrier(jnp.mean(center * center, axis=-1, keepdims=True)) + 1e-05)
    normal_form = center * inv_scale
    normed = (normal_form * gain + bias).astype(jnp.bfloat16)
    pre_act = jnp.dot(normed, w_in, preferred_element_type=jnp.float32) + b_in
    hidden = (pre_act * jax.nn.sigmoid(pre_act)).astype(jnp.bfloat16)
    updated = (summed + jnp.dot(hidden, w_out, preferred_element_type=jnp.float32)).astype(jnp.bfloat16)
    return (normal_form, inv_scale, normed, pre_act, hidden, updated)

def pair_backward(sym, bin_labels, parts, gain, w_in, w_out, w_bins):
    normal_form, inv_scale, normed, pre_act, hidden, updated = parts
    shifted = sym - lax.optimization_barrier(jnp.max(sym, axis=-1, keepdims=True))
    expo = jnp.exp(shifted)
    probs = expo / lax.optimization_barrier(jnp.sum(expo, axis=-1, keepdims=True))
    onehot = (bin_labels[..., None] == lax.iota(jnp.int32, sym.shape[-1])).astype(jnp.float32)
    logit_grad = (2.0 * (probs - onehot)).reshape(-1, sym.shape[-1]).astype(jnp.bfloat16)
    grad_bins = inner(updated, logit_grad)
    upd_grad = outer(logit_grad, w_bins)
    upd_half = upd_grad.astype(jnp.bfloat16)
    grad_out = inner(hidden, upd_half)
    hid_grad = outer(upd_half, w_out)
    sigma = jax.nn.sigmoid(pre_act)
    pre_grad = (hid_grad * sigma * (1.0 + pre_act * (1.0 - sigma))).astype(jnp.bfloat16)
    grad_in = inner(normed, pre_grad)
    norm_grad = outer(pre_grad, w_in) * gain
    pair_grad = inv_scale * (norm_grad - lax.optimization_barrier(jnp.mean(norm_grad, axis=-1, keepdims=True)) - normal_form * lax.optimization_barrier(jnp.mean(norm_grad * normal_form, axis=-1, keepdims=True))) + upd_grad
    return (grad_in, grad_out, grad_bins, pair_grad)

def reference(left_act, right_act, norm_gain, norm_bias, w_in, b_in, w_out, w_bins, labels):
    residues, width = left_act.shape
    stride_rows = 8
    groups = residues // stride_rows
    left_groups = left_act.reshape(groups, stride_rows, width)
    right_groups = right_act.reshape(groups, stride_rows, width)

    def forward(record):
        parts = transition(record[0], right_act, norm_gain, norm_bias, w_in, b_in, w_out)
        return jnp.dot(parts[5], w_bins, preferred_element_type=jnp.float32).reshape(stride_rows, residues, -1)
    logits = lax.map(forward, (left_groups, right_groups)).reshape(residues, residues, -1)

    def advance(running, record):
        position, left_rows, bin_labels = record
        own = lax.dynamic_slice_in_dim(logits, position * stride_rows, stride_rows, 0)
        far = jnp.transpose(lax.dynamic_slice_in_dim(logits, position * stride_rows, stride_rows, 1), (1, 0, 2))
        parts = transition(left_rows, right_act, norm_gain, norm_bias, w_in, b_in, w_out)
        grads = pair_backward(own + far, bin_labels, parts, norm_gain, w_in, w_out, w_bins)
        pair_grad = grads[3].reshape(stride_rows, residues, width)
        running = (running[0] + grads[0], running[1] + grads[1], running[2] + grads[2], running[3] + lax.optimization_barrier(jnp.sum(pair_grad, axis=0)))
        return (running, lax.optimization_barrier(jnp.sum(pair_grad, axis=1)))
    start = (jnp.zeros((width, w_in.shape[1]), jnp.float32), jnp.zeros((w_in.shape[1], width), jnp.float32), jnp.zeros((width, w_bins.shape[1]), jnp.float32), jnp.zeros((residues, width), jnp.float32))
    positions = jnp.arange(groups, dtype=jnp.int32)
    running, left_terms = lax.scan(advance, start, (positions, left_groups, labels.reshape(groups, stride_rows, residues)))
    grad_left = left_terms.reshape(residues, width)
    return (grad_left, running[3], running[0] / residues, running[1] / residues, running[2] / residues)
```

```python
import functools

import jax
import jax.numpy as jnp
from jax import lax
from jax.experimental import pallas as pl
from jax.experimental.pallas import tpu as pltpu
from jax.sharding import PartitionSpec as P

GROUP = 8
F32 = jnp.float32
BF16 = jnp.bfloat16


def from_everyone(value, axis):
    count = lax.axis_size(axis)
    return lax.all_to_all(
        jnp.broadcast_to(value[None], (count, *value.shape)), axis, 0, 0, tiled=True
    )


def inner(first, second):
    return lax.dot_general(first, second, (((0,), (0,)), ((), ())), preferred_element_type=F32)


def dot(first, second):
    return jnp.dot(first, second, preferred_element_type=F32)


def pair_kernel(
    place,
    from_row_mates,
    from_col_mates,
    gain_ref,
    bias_ref,
    w_in_ref,
    b_in_ref,
    w_out_ref,
    w_bins_ref,
    w_in_t_ref,
    w_out_t_ref,
    w_bins_t_ref,
    col_out,
    row_out,
    own_out,
    blk,
    blk_center,
    far_side,
    far_center,
    label_rows,
    grad_in,
    grad_out_t,
    grad_bins,
    blk_sums,
    side_sums,
    *,
    count,
    rows,
):
    block = count * rows
    half = block // 2
    width = gain_ref.shape[1]
    row_at = place[0]
    col_at = place[1]

    for m in range(count):
        for side in range(2):
            blk[side, m * rows : (m + 1) * rows, :] = from_row_mates[
                m, rows * (1 + side) : rows * (2 + side), :
            ]
    far_side[...] = jnp.zeros_like(far_side)
    label_rows[...] = jnp.zeros_like(label_rows)
    for m in range(count // 2 + 1):
        source = lax.rem(row_at + m, count)
        for side in range(2):
            far_side[side, m * rows : (m + 1) * rows, :] = from_col_mates[
                source, rows * side : rows * (side + 1), :
            ]
        label_rows[m * rows : (m + 1) * rows, :] = from_row_mates[source, 0:rows, :]
    if rows < GROUP:
        for side in range(2):
            far_side[side, half + rows : half + GROUP, :] = far_side[side, rows:GROUP, :]
        label_rows[half + rows : half + GROUP, :] = label_rows[rows:GROUP, :]
    for side in range(2):
        value = blk[side]
        blk_center[side] = value - jnp.mean(value, axis=-1, keepdims=True)
        value = far_side[side]
        far_center[side] = value - jnp.mean(value, axis=-1, keepdims=True)

    grad_in[...] = jnp.zeros_like(grad_in)
    grad_out_t[...] = jnp.zeros_like(grad_out_t)
    grad_bins[...] = jnp.zeros_like(grad_bins)
    side_sums[...] = jnp.zeros_like(side_sums)

    gain = gain_ref[...]
    bias = bias_ref[...]
    sub = lax.broadcasted_iota(jnp.int32, (GROUP, width), 0)
    lane = lax.broadcasted_iota(jnp.int32, (GROUP, width), 1)
    bin_lane = lax.broadcasted_iota(jnp.int32, (GROUP, w_bins_ref.shape[1]), 1).astype(F32)
    own_at = rows * col_at + sub
    span = GROUP * half
    every = span + GROUP

    apart_label = jnp.sum(
        jnp.where(lane == own_at, label_rows[half : half + GROUP, :], 0.0), axis=-1, keepdims=True
    )

    def step(s, carry):
        first = pl.multiple_of(s * GROUP, GROUP)
        eight = [blk[side, pl.ds(first, GROUP), :] for side in range(2)]
        eight_center = [blk_center[side, pl.ds(first, GROUP), :] for side in range(2)]
        near = [(sub >= rows) | (own_at >= first + ii) for ii in range(GROUP)]

        def listed(ref, mask, *lead):
            head = jnp.where(
                mask, ref[(*lead, slice(0, GROUP))], ref[(*lead, slice(half, half + GROUP))]
            )
            return head

        summed, center = [], []
        for side in range(2):
            for ii in range(GROUP):
                for source, own, into in (
                    (far_side, eight, summed),
                    (far_center, eight_center, center),
                ):
                    one = own[side][ii : ii + 1, :]
                    into.append(listed(source, near[ii], 1 - side) + one)
                    if half > GROUP:
                        into.append(source[1 - side, GROUP:half, :] + one)
            for source, into in ((far_side, summed), (far_center, center)):
                into.append(source[side, 0:GROUP, :] + source[1 - side, half : half + GROUP, :])
        summed = jnp.concatenate(summed, axis=0)
        center = jnp.concatenate(center, axis=0)
        inv_scale = lax.rsqrt(jnp.mean(center * center, axis=-1, keepdims=True) + 1e-05)
        normal_form = center * inv_scale
        normed = (normal_form * gain + bias).astype(BF16)
        act = dot(normed, w_in_ref[...]) + b_in_ref[...]
        up = jnp.tanh(act) + 1.0
        hidden = (act * up).astype(BF16)
        slope = up * (act * (2.0 - up) + 1.0)
        updated = (summed + dot(hidden, w_out_ref[...])).astype(BF16)
        logits = dot(updated, w_bins_ref[...])
        sym = logits[0:every] + logits[every:]

        hots, scales = [], []
        rest = jnp.full((half - GROUP, 1), 2.0, F32) if half > GROUP else None
        for ii in range(GROUP):
            picked = []
            for lo, hi in ((0, GROUP), (half, half + GROUP)):
                picked.append(
                    jnp.sum(
                        jnp.where(lane == first + ii, label_rows[lo:hi, :], 0.0),
                        axis=-1,
                        keepdims=True,
                    )
                )
            hots.append(jnp.where(near[ii][:, 0:1], picked[0], picked[1]))
            own = (own_at[:, 0:1] == first + ii) & (sub[:, 0:1] < rows)
            scales.append(jnp.where(own, 1.0, 2.0))
            if half > GROUP:
                wide = lax.broadcasted_iota(jnp.int32, (half - GROUP, width), 1)
                hots.append(
                    jnp.sum(
                        jnp.where(wide == first + ii, label_rows[GROUP:half, :], 0.0),
                        axis=-1,
                        keepdims=True,
                    )
                )
                scales.append(rest)
        hots.append(apart_label)
        scales.append(jnp.where((sub[:, 0:1] < rows) & (s == 0), 1.0, 0.0))
        hot = jnp.concatenate(hots, axis=0)
        scale = jnp.concatenate(scales, axis=0)
        lanes = jnp.broadcast_to(bin_lane[0:1], sym.shape)
        expo = jnp.exp(sym - jnp.max(sym, axis=-1, keepdims=True))
        probs = expo / jnp.sum(expo, axis=-1, keepdims=True)
        logit_grad = (scale * (probs - jnp.where(lanes == hot, 1.0, 0.0))).astype(BF16)

        upd_grad = dot(logit_grad, w_bins_t_ref[...])
        upd_half = upd_grad.astype(BF16)
        grad_bins[...] += inner(updated[0:every], logit_grad) + inner(updated[every:], logit_grad)
        grad_out_t[...] += inner(upd_half, hidden[0:every]) + inner(upd_half, hidden[every:])
        hid_grad = dot(upd_half, w_out_t_ref[...])
        pre_grad = jnp.concatenate(
            [(hid_grad * slope[0:every]).astype(BF16), (hid_grad * slope[every:]).astype(BF16)],
            axis=0,
        )
        grad_in[...] += inner(normed, pre_grad)
        norm_grad = dot(pre_grad, w_in_t_ref[...]) * gain
        pair_grad = inv_scale * (
            norm_grad
            - jnp.mean(norm_grad, axis=-1, keepdims=True)
            - normal_form * jnp.mean(norm_grad * normal_form, axis=-1, keepdims=True)
        )
        for side in range(2):
            mine = pair_grad[side * every : (side + 1) * every] + upd_grad
            ones, head_near, head_far, tail = [], None, None, None
            for ii in range(GROUP):
                part = mine[ii * half : (ii + 1) * half]
                ones.append(jnp.sum(part, axis=0, keepdims=True))
                close = jnp.where(near[ii], part[0:GROUP], 0.0)
                away = part[0:GROUP] - close
                head_near = close if ii == 0 else head_near + close
                head_far = away if ii == 0 else head_far + away
                if half > GROUP:
                    tail = part[GROUP:] if ii == 0 else tail + part[GROUP:]
            blk_sums[side, pl.ds(first, GROUP), :] = jnp.concatenate(ones, axis=0)
            side_sums[1 - side, 0:GROUP, :] += head_near
            side_sums[1 - side, half : half + GROUP, :] += head_far
            if half > GROUP:
                side_sums[1 - side, GROUP:half, :] += tail
            side_sums[side, half + GROUP : half + 2 * GROUP, :] += mine[span:]
            side_sums[1 - side, half : half + GROUP, :] += mine[span:]
        return carry

    lax.fori_loop(0, block // GROUP, step, 0)

    share_in = grad_in.shape[0] // count
    share_out = grad_out_t.shape[1] // count
    tiles = grad_in.shape[1] // width
    grad_out = grad_out_t[...].T
    bins = grad_bins[...]
    bins = jnp.concatenate([bins, jnp.zeros_like(bins)], axis=1)
    for m in range(count):
        at = 0
        for t in range(tiles):
            col_out[m, at : at + share_in, :] = grad_in[
                m * share_in : (m + 1) * share_in, t * width : (t + 1) * width
            ]
            at += share_in
        col_out[m, at : at + share_out, :] = grad_out[m * share_out : (m + 1) * share_out]
        at += share_out
        col_out[m, at : at + share_in, :] = bins[m * share_in : (m + 1) * share_in]
        at += share_in
        for side in range(2):
            col_out[m, at : at + GROUP, :] = jnp.zeros((GROUP, width), F32)
            col_out[m, at : at + rows, :] = blk_sums[side, m * rows : (m + 1) * rows, :]
            at += GROUP
    row_out[...] = jnp.zeros_like(row_out)
    for m in range(count // 2 + 1):
        target = lax.rem(row_at + m, count)
        for side in range(2):
            row_out[target, side * GROUP : side * GROUP + rows, :] = side_sums[
                side, m * rows : (m + 1) * rows, :
            ]
    for side in range(2):
        own_out[side * GROUP : (side + 1) * GROUP, :] = side_sums[
            side, half + GROUP : half + 2 * GROUP, :
        ]


def run_pairs(place, from_row_mates, from_col_mates, gain, bias, w_in, b_in, w_out, w_bins):
    count = from_row_mates.shape[0]
    rows = from_row_mates.shape[1] // 3
    width, hidden = w_in.shape
    bins = w_bins.shape[1]
    block = count * rows
    half = block // 2
    share = (width // count) * (hidden // width) + hidden // count + width // count
    vmem = pl.BlockSpec(memory_space=pltpu.VMEM)
    smem = pl.BlockSpec(memory_space=pltpu.SMEM)
    halved = w_in * jnp.asarray(0.5, BF16)
    return pl.pallas_call(
        functools.partial(pair_kernel, count=count, rows=rows),
        out_shape=(
            jax.ShapeDtypeStruct((count, share + 2 * GROUP, width), F32),
            jax.ShapeDtypeStruct((count, 2 * GROUP, width), F32),
            jax.ShapeDtypeStruct((2 * GROUP, width), F32),
        ),
        in_specs=[smem] + [vmem] * 11,
        out_specs=(vmem, vmem, vmem),
        scratch_shapes=[
            pltpu.VMEM((2, block, width), F32),
            pltpu.VMEM((2, block, width), F32),
            pltpu.VMEM((2, half + GROUP, width), F32),
            pltpu.VMEM((2, half + GROUP, width), F32),
            pltpu.VMEM((half + GROUP, width), F32),
            pltpu.VMEM((width, hidden), F32),
            pltpu.VMEM((width, hidden), F32),
            pltpu.VMEM((width, bins), F32),
            pltpu.VMEM((2, block, width), F32),
            pltpu.VMEM((2, half + 2 * GROUP, width), F32),
        ],
        compiler_params=pltpu.CompilerParams(vmem_limit_bytes=56 * 1024 * 1024),
        interpret=INTERPRET,
        name="pairs",
    )(
        place,
        from_row_mates.astype(F32),
        from_col_mates.astype(F32),
        gain[None],
        bias[None],
        halved,
        0.5 * b_in[None],
        w_out,
        w_bins,
        w_in.T,
        w_out.T * jnp.asarray(0.5, BF16),
        w_bins.T,
    )


INTERPRET = False


def on_device(left_act, right_act, norm_gain, norm_bias, w_in, b_in, w_out, w_bins, labels):
    count = lax.axis_size("col")
    rows, width = left_act.shape
    hidden = w_in.shape[1]
    row_at = lax.axis_index("row")
    col_at = lax.axis_index("col")
    stacked = jnp.concatenate([left_act, right_act], axis=0)
    turned = jnp.pad(labels.T.astype(BF16), ((0, 0), (0, width - labels.shape[0])))
    to_row_mates = jnp.concatenate(
        [
            turned.reshape(count, rows, width),
            jnp.broadcast_to(stacked[None], (count, 2 * rows, width)),
        ],
        axis=1,
    )
    from_row_mates = lax.all_to_all(to_row_mates, "col", 0, 0, tiled=True)
    from_col_mates = from_everyone(stacked, "row")
    place = jnp.stack([row_at, col_at]).astype(jnp.int32)
    col_out, row_out, own_out = run_pairs(
        place, from_row_mates, from_col_mates, norm_gain, norm_bias, w_in, b_in, w_out, w_bins
    )
    by_col = lax.all_to_all(col_out, "col", 0, 0, tiled=True).sum(axis=0)
    by_row = lax.all_to_all(row_out, "row", 0, 0, tiled=True).sum(axis=0)
    share = by_col.shape[0] - 2 * GROUP
    both = by_col[share:] + by_row + own_out
    grad_left = both[0:rows]
    size = lax.axis_size("row")
    swap = [(a * count + b, b * count + a) for a in range(size) for b in range(count)]
    right = lax.ppermute(both[GROUP:], ("row", "col"), swap)
    weights = from_everyone(by_col[0:share], "row").sum(axis=0) / (rows * count * size)
    grad_right = from_everyone(right, "row")[:, 0:rows].reshape(rows * size, width)
    weights = from_everyone(weights, "col")
    cut = (width // count) * (hidden // width)
    grad_in = (
        weights[:, 0:cut]
        .reshape(count, hidden // width, width // count, width)
        .transpose(0, 2, 1, 3)
        .reshape(width, hidden)
    )
    grad_out = weights[:, cut : cut + hidden // count].reshape(hidden, width)
    grad_bins = weights[:, cut + hidden // count :, 0 : w_bins.shape[1]].reshape(width, -1)
    return (grad_left, grad_right, grad_in, grad_out, grad_bins)


def solution(mesh):
    placed = (
        P(("row", "col"), None),
        P(("row", "col"), None),
        P(),
        P(),
        P(),
        P(),
        P(),
        P(),
        P("row", "col"),
    )
    return jax.shard_map(
        on_device,
        mesh=mesh,
        in_specs=placed,
        out_specs=(P(("row", "col"), None), P("col", None), P(), P(), P()),
        check_vma=False,
    )
```

```python
import functools

import jax
import jax.numpy as jnp
from jax import lax
from jax.experimental import pallas as pl
from jax.experimental.pallas import tpu as pltpu
from jax.sharding import PartitionSpec as P

GROUP = 8
F32 = jnp.float32
BF16 = jnp.bfloat16


def from_everyone(value, axis):
    count = lax.axis_size(axis)
    return lax.all_to_all(
        jnp.broadcast_to(value[None], (count, *value.shape)), axis, 0, 0, tiled=True
    )


def inner(first, second):
    return lax.dot_general(first, second, (((0,), (0,)), ((), ())), preferred_element_type=F32)


def dot(first, second):
    return jnp.dot(first, second, preferred_element_type=F32)


def pair_kernel(
    place,
    mine_ref,
    theirs_ref,
    labels_ref,
    gain_ref,
    bias_ref,
    w_in_ref,
    b_in_ref,
    w_out_ref,
    w_bins_ref,
    w_in_t_ref,
    w_out_t_ref,
    w_bins_t_ref,
    weight_out,
    kept_out,
    sent_out,
    blk,
    blk_center,
    far_side,
    far_center,
    label_rows,
    grad_in,
    grad_out_t,
    grad_bins,
    side_sums,
    *,
    count,
    rows,
):
    block = count * rows
    half = block // 2
    width = gain_ref.shape[1]
    beyond = half + GROUP
    twin = place[0] == place[1]
    skew = (place[0] > place[1]).astype(jnp.int32)

    for m in range(count):
        one = mine_ref[m].astype(F32)
        other = theirs_ref[m].astype(F32)
        for side in range(2):
            at = side * GROUP
            blk[side, m * rows : (m + 1) * rows, :] = one[at : at + rows]
            far_side[side, m * rows : (m + 1) * rows, :] = other[at : at + rows]
    label_rows[0:block, :] = labels_ref[...]
    label_rows[block:, :] = labels_ref[0:beyond, :]
    for side in range(2):
        value = blk[side]
        blk_center[side] = value - jnp.mean(value, axis=-1, keepdims=True)
        value = far_side[side, 0:block, :]
        value = value - jnp.mean(value, axis=-1, keepdims=True)
        far_center[side, 0:block, :] = value
        far_center[side, block:, :] = value[0:beyond]
        far_side[side, block:, :] = far_side[side, 0:beyond, :]

    grad_in[...] = jnp.zeros_like(grad_in)
    grad_out_t[...] = jnp.zeros_like(grad_out_t)
    grad_bins[...] = jnp.zeros_like(grad_bins)
    side_sums[...] = jnp.zeros_like(side_sums)

    gain = gain_ref[...]
    bias = bias_ref[...]
    sub = lax.broadcasted_iota(jnp.int32, (GROUP, width), 0)
    lane = lax.broadcasted_iota(jnp.int32, (GROUP, width), 1)
    near = [sub >= ii + skew for ii in range(GROUP)]
    bin_lane = lax.broadcasted_iota(jnp.int32, (GROUP, w_bins_ref.shape[1]), 1).astype(F32)
    span = GROUP * half
    every = span + GROUP

    def step(s, carry):
        first = pl.multiple_of(s * GROUP, GROUP)

        def head(ref, *lead):
            return ref[(*lead, pl.ds(first, GROUP), slice(None))]

        def middle(ref, *lead):
            return ref[(*lead, pl.ds(first + GROUP, half - GROUP), slice(None))]

        def away(ref, *lead):
            return ref[(*lead, pl.ds(first + half, GROUP), slice(None))]

        summed, center = [], []
        for mine, other, into in ((blk, far_side, summed), (blk_center, far_center, center)):
            for side in range(2):
                own = head(mine, side)
                close, apart = head(other, 1 - side), away(other, 1 - side)
                rest = middle(other, 1 - side) if half > GROUP else None
                for ii in range(GROUP):
                    one = own[ii : ii + 1, :]
                    into.append(jnp.where(near[ii], close, apart) + one)
                    if half > GROUP:
                        into.append(rest + one)
                into.append(own + apart)
        summed = jnp.concatenate(summed, axis=0)
        center = jnp.concatenate(center, axis=0)
        inv_scale = lax.rsqrt(jnp.mean(center * center, axis=-1, keepdims=True) + 1e-05)
        normal_form = center * inv_scale
        normed = (normal_form * gain + bias).astype(BF16)
        act = dot(normed, w_in_ref[...]) + b_in_ref[...]
        up = jnp.tanh(act) + 1.0
        hidden = (act * up).astype(BF16)
        slope = up * (act * (2.0 - up) + 1.0)
        updated = (summed + dot(hidden, w_out_ref[...])).astype(BF16)
        logits = dot(updated, w_bins_ref[...])
        sym = logits[0:every] + logits[every:]

        hots, scales = [], []
        label_close, label_apart = head(label_rows), away(label_rows)
        if half > GROUP:
            label_rest = middle(label_rows)
            wide = lax.broadcasted_iota(jnp.int32, label_rest.shape, 1)
            plain = jnp.full((half - GROUP, 1), 2.0, F32)
        for ii in range(GROUP):
            chosen = jnp.where(near[ii], label_close, label_apart)
            hots.append(
                jnp.sum(jnp.where(lane == first + ii, chosen, 0.0), axis=-1, keepdims=True)
            )
            scales.append(jnp.where((sub[:, 0:1] == ii) & twin, 1.0, 2.0))
            if half > GROUP:
                hots.append(
                    jnp.sum(jnp.where(wide == first + ii, label_rest, 0.0), axis=-1, keepdims=True)
                )
                scales.append(plain)
        hots.append(
            jnp.sum(jnp.where(lane == first + sub, label_apart, 0.0), axis=-1, keepdims=True)
        )
        scales.append(jnp.where((sub[:, 0:1] >= 0) & twin, 1.0, 0.0))
        hot = jnp.concatenate(hots, axis=0)
        scale = jnp.concatenate(scales, axis=0)
        lanes = jnp.broadcast_to(bin_lane[0:1], sym.shape)
        expo = jnp.exp(sym - jnp.max(sym, axis=-1, keepdims=True))
        probs = expo / jnp.sum(expo, axis=-1, keepdims=True)
        logit_grad = (scale * (probs - jnp.where(lanes == hot, 1.0, 0.0))).astype(BF16)

        upd_grad = dot(logit_grad, w_bins_t_ref[...])
        upd_half = upd_grad.astype(BF16)
        grad_bins[...] += inner(updated[0:every], logit_grad) + inner(updated[every:], logit_grad)
        grad_out_t[...] += inner(upd_half, hidden[0:every]) + inner(upd_half, hidden[every:])
        hid_grad = dot(upd_half, w_out_t_ref[...])
        pre_grad = jnp.concatenate(
            [(hid_grad * slope[0:every]).astype(BF16), (hid_grad * slope[every:]).astype(BF16)],
            axis=0,
        )
        grad_in[...] += inner(normed, pre_grad)
        norm_grad = dot(pre_grad, w_in_t_ref[...]) * gain
        pair_grad = inv_scale * (
            norm_grad
            - jnp.mean(norm_grad, axis=-1, keepdims=True)
            - normal_form * jnp.mean(norm_grad * normal_form, axis=-1, keepdims=True)
        )
        for side in range(2):
            mine = pair_grad[side * every : (side + 1) * every] + upd_grad
            ones, head_near, head_far, tail = [], None, None, None
            for ii in range(GROUP):
                part = mine[ii * half : (ii + 1) * half]
                ones.append(jnp.sum(part, axis=0, keepdims=True))
                close = jnp.where(near[ii], part[0:GROUP], 0.0)
                apart = part[0:GROUP] - close
                head_near = close if ii == 0 else head_near + close
                head_far = apart if ii == 0 else head_far + apart
                if half > GROUP:
                    tail = part[GROUP:] if ii == 0 else tail + part[GROUP:]
            target = kept_out if side == 0 else sent_out
            target[side, pl.ds(first, GROUP), :] = jnp.concatenate(ones, axis=0) + mine[span:]
            side_sums[1 - side, pl.ds(first, GROUP), :] += head_near
            side_sums[1 - side, pl.ds(first + half, GROUP), :] += head_far + mine[span:]
            if half > GROUP:
                side_sums[1 - side, pl.ds(first + GROUP, half - GROUP), :] += tail
        return carry

    lax.fori_loop(0, block // GROUP, step, 0)

    for side in range(2):
        target = sent_out if side == 0 else kept_out
        target[side, 0:beyond, :] = side_sums[side, 0:beyond, :] + side_sums[side, block:, :]
        target[side, beyond:, :] = side_sums[side, beyond:block, :]

    share_in = grad_in.shape[0] // count
    share_out = grad_out_t.shape[1] // count
    tiles = grad_in.shape[1] // width
    grad_out = grad_out_t[...].T
    bins = grad_bins[...]
    bins = jnp.concatenate([bins, jnp.zeros_like(bins)], axis=1)
    for m in range(count):
        at = 0
        for t in range(tiles):
            weight_out[m, at : at + share_in, :] = grad_in[
                m * share_in : (m + 1) * share_in, t * width : (t + 1) * width
            ]
            at += share_in
        weight_out[m, at : at + share_out, :] = grad_out[m * share_out : (m + 1) * share_out]
        at += share_out
        weight_out[m, at : at + share_in, :] = bins[m * share_in : (m + 1) * share_in]


def run_pairs(place, mine, theirs, rows, labels, gain, bias, w_in, b_in, w_out, w_bins):
    count = mine.shape[0]
    width, hidden = w_in.shape
    bins = w_bins.shape[1]
    block = count * rows
    long = block + block // 2 + GROUP
    share = (width // count) * (hidden // width) + hidden // count + width // count
    vmem = pl.BlockSpec(memory_space=pltpu.VMEM)
    smem = pl.BlockSpec(memory_space=pltpu.SMEM)
    return pl.pallas_call(
        functools.partial(pair_kernel, count=count, rows=rows),
        out_shape=(
            jax.ShapeDtypeStruct((count, share, width), F32),
            jax.ShapeDtypeStruct((2, block, width), F32),
            jax.ShapeDtypeStruct((2, block, width), F32),
        ),
        in_specs=[smem] + [vmem] * 12,
        out_specs=(vmem, vmem, vmem),
        scratch_shapes=[
            pltpu.VMEM((2, block, width), F32),
            pltpu.VMEM((2, block, width), F32),
            pltpu.VMEM((2, long, width), F32),
            pltpu.VMEM((2, long, width), F32),
            pltpu.VMEM((long, width), F32),
            pltpu.VMEM((width, hidden), F32),
            pltpu.VMEM((width, hidden), F32),
            pltpu.VMEM((width, bins), F32),
            pltpu.VMEM((2, long, width), F32),
        ],
        compiler_params=pltpu.CompilerParams(vmem_limit_bytes=56 * 1024 * 1024),
        interpret=INTERPRET,
        name="pairs",
    )(
        place,
        mine,
        theirs,
        labels,
        gain[None],
        bias[None],
        w_in * jnp.asarray(0.5, BF16),
        0.5 * b_in[None],
        w_out,
        w_bins,
        w_in.T,
        w_out.T * jnp.asarray(0.5, BF16),
        w_bins.T,
    )


INTERPRET = False


def on_device(left_act, right_act, norm_gain, norm_bias, w_in, b_in, w_out, w_bins, labels):
    count = lax.axis_size("col")
    size = lax.axis_size("row")
    rows, width = left_act.shape
    hidden = w_in.shape[1]
    swap = [(a * count + b, b * count + a) for a in range(size) for b in range(count)]
    gap = jnp.zeros((GROUP - rows, width), left_act.dtype)
    stacked = jnp.concatenate([left_act, gap, right_act, gap], axis=0)
    mine = from_everyone(stacked, "col")
    theirs = lax.ppermute(mine, ("row", "col"), swap)
    turned = jnp.pad(labels.T.astype(F32), ((0, 0), (0, width - labels.shape[0])))
    place = jnp.stack([lax.axis_index("row"), lax.axis_index("col")]).astype(jnp.int32)
    weight_out, kept, sent = run_pairs(
        place, mine, theirs, rows, turned, norm_gain, norm_bias, w_in, b_in, w_out, w_bins
    )
    kept = kept + lax.ppermute(sent, ("row", "col"), swap)
    shares = lax.all_to_all(weight_out, "col", 0, 0, tiled=True).sum(axis=0)
    share = shares.shape[0]
    piece = -(-share // size)
    shares = jnp.pad(shares, ((0, piece * size - share), (0, 0)))
    pieces = jnp.concatenate(
        [shares.reshape(size, piece, width), kept[1].reshape(size, rows, width)], axis=1
    )
    pieces = lax.all_to_all(pieces, "row", 0, 0, tiled=True).sum(axis=0)
    scale = jnp.where(
        lax.broadcasted_iota(jnp.int32, pieces.shape, 0) < piece, 1.0 / (rows * count * size), 1.0
    )
    pieces = from_everyone(pieces * scale, "row")
    grad_right = pieces[:, piece:].reshape(rows * size, width)
    shares = pieces[:, 0:piece].reshape(size * piece, width)[0:share]
    last = jnp.concatenate(
        [
            jnp.broadcast_to(shares[None], (count, share, width)),
            kept[0].reshape(count, rows, width),
        ],
        axis=1,
    )
    last = lax.all_to_all(last, "col", 0, 0, tiled=True)
    grad_left = last[:, share:].sum(axis=0)
    cut = (width // count) * (hidden // width)
    grad_in = (
        last[:, 0:cut]
        .reshape(count, hidden // width, width // count, width)
        .transpose(0, 2, 1, 3)
        .reshape(width, hidden)
    )
    grad_out = last[:, cut : cut + hidden // count].reshape(hidden, width)
    grad_bins = last[:, cut + hidden // count : share, 0 : w_bins.shape[1]].reshape(width, -1)
    return (grad_left, grad_right, grad_in, grad_out, grad_bins)


def solution(mesh):
    placed = (
        P(("row", "col"), None),
        P(("row", "col"), None),
        P(),
        P(),
        P(),
        P(),
        P(),
        P(),
        P("row", "col"),
    )
    return jax.shard_map(
        on_device,
        mesh=mesh,
        in_specs=placed,
        out_specs=(P(("row", "col"), None), P("col", None), P(), P(), P()),
        check_vma=False,
    )
```

```python
import functools

import jax
import jax.numpy as jnp
from jax import lax
from jax.experimental import pallas as pl
from jax.experimental.pallas import tpu as pltpu
from jax.sharding import PartitionSpec as P


GROUP = 8
F32 = jnp.float32
BF16 = jnp.bfloat16


def from_everyone(value, axis):
    count = lax.axis_size(axis)
    return lax.all_to_all(
        jnp.broadcast_to(value[None], (count, *value.shape)), axis, 0, 0, tiled=True
    )


def inner(first, second):
    return lax.dot_general(first, second, (((0,), (0,)), ((), ())), preferred_element_type=F32)


def outer(first, second):
    return lax.dot_general(first, second, (((1,), (1,)), ((), ())), preferred_element_type=F32)


def dot(first, second):
    return jnp.dot(first, second, preferred_element_type=F32)


def twin_swap(size, count):
    return [(a * count + b, b * count + a) for a in range(size) for b in range(count)]


def block_routes(size, count):
    if (size, count) != (16, 16):
        return twin_swap(size, count)
    pairs = []
    for r in range(size):
        for c in range(count):
            y, z = (r // 4 - c // 4) % 4, (r % 4 - c % 4) % 4
            low = (c // 2) % 2
            low = (low, 1, 1 - low, 0)[z]
            k = 4 * ((c // 4 + 2 - y) % 4) + 2 * low + (z + 1) % 2
            pairs.append((c * count + k, r * count + c))
    return pairs


def pair_kernel(
    place,
    mine_ref,
    theirs_ref,
    labels_ref,
    gain_ref,
    bias_ref,
    w_in_ref,
    b_in_ref,
    w_out_ref,
    w_bins_ref,
    col_out,
    row_out,
    w_in_half,
    w_out_half,
    blk,
    blk_center,
    far_side,
    far_center,
    label_rows,
    grad_in,
    grad_out_t,
    grad_bins,
    blk_sums,
    side_sums,
    *,
    count,
    rows,
):
    block = count * rows
    half = block // 2
    width = gain_ref.shape[1]
    beyond = half + GROUP
    twin = place[0] == place[1]
    skew = (place[0] > place[1]).astype(jnp.int32)

    for m in range(count):
        one = mine_ref[m].astype(F32)
        other = theirs_ref[m].astype(F32)
        for side in range(2):
            at = side * GROUP
            blk[side, m * rows : (m + 1) * rows, :] = one[at : at + rows]
            far_side[side, m * rows : (m + 1) * rows, :] = other[at : at + rows]
    label_rows[0:block, :] = labels_ref[...]
    label_rows[block:, :] = labels_ref[0:beyond, :]
    for side in range(2):
        value = blk[side]
        blk_center[side] = value - jnp.mean(value, axis=-1, keepdims=True)
        value = far_side[side, 0:block, :]
        value = value - jnp.mean(value, axis=-1, keepdims=True)
        far_center[side, 0:block, :] = value
        far_center[side, block:, :] = value[0:beyond]
        far_side[side, block:, :] = far_side[side, 0:beyond, :]

    grad_in[...] = jnp.zeros_like(grad_in)
    grad_out_t[...] = jnp.zeros_like(grad_out_t)
    grad_bins[...] = jnp.zeros_like(grad_bins)
    side_sums[...] = jnp.zeros_like(side_sums)

    w_in_half[...] = w_in_ref[...] * jnp.asarray(0.5, BF16)
    w_out_half[...] = w_out_ref[...] * jnp.asarray(0.5, BF16)
    gain = gain_ref[...]
    bias = bias_ref[...]
    b_in = 0.5 * b_in_ref[...]
    sub = lax.broadcasted_iota(jnp.int32, (GROUP, width), 0)
    lane = lax.broadcasted_iota(jnp.int32, (GROUP, width), 1)
    near = [sub >= ii + skew for ii in range(GROUP)]
    bin_lane = lax.broadcasted_iota(jnp.int32, (GROUP, w_bins_ref.shape[1]), 1).astype(F32)
    span = GROUP * half
    every = span + GROUP

    def step(s, carry):
        first = pl.multiple_of(s * GROUP, GROUP)

        def head(ref, *lead):
            return ref[(*lead, pl.ds(first, GROUP), slice(None))]

        def middle(ref, *lead):
            return ref[(*lead, pl.ds(first + GROUP, half - GROUP), slice(None))]

        def away(ref, *lead):
            return ref[(*lead, pl.ds(first + half, GROUP), slice(None))]

        summed, center = [], []
        for mine, other, into in ((blk, far_side, summed), (blk_center, far_center, center)):
            for side in range(2):
                own = head(mine, side)
                close, apart = head(other, 1 - side), away(other, 1 - side)
                rest = middle(other, 1 - side) if half > GROUP else None
                for ii in range(GROUP):
                    one = own[ii : ii + 1, :]
                    into.append(jnp.where(near[ii], close, apart) + one)
                    if half > GROUP:
                        into.append(rest + one)
                into.append(own + apart)
        summed = jnp.concatenate(summed, axis=0)
        center = jnp.concatenate(center, axis=0)
        inv_scale = lax.rsqrt(jnp.mean(center * center, axis=-1, keepdims=True) + 1e-05)
        normal_form = center * inv_scale
        normed = (normal_form * gain + bias).astype(BF16)
        act = dot(normed, w_in_half[...]) + b_in
        up = jnp.tanh(act) + 1.0
        hidden = (act * up).astype(BF16)
        slope = up * (act * (2.0 - up) + 1.0)
        updated = (summed + dot(hidden, w_out_ref[...])).astype(BF16)
        logits = dot(updated, w_bins_ref[...])
        sym = logits[0:every] + logits[every:]

        hots, scales = [], []
        label_close, label_apart = head(label_rows), away(label_rows)
        if half > GROUP:
            label_rest = middle(label_rows)
            wide = lax.broadcasted_iota(jnp.int32, label_rest.shape, 1)
            plain = jnp.full((half - GROUP, 1), 2.0, F32)
        for ii in range(GROUP):
            chosen = jnp.where(near[ii], label_close, label_apart)
            hots.append(
                jnp.sum(jnp.where(lane == first + ii, chosen, 0.0), axis=-1, keepdims=True)
            )
            scales.append(jnp.where((sub[:, 0:1] == ii) & twin, 1.0, 2.0))
            if half > GROUP:
                hots.append(
                    jnp.sum(jnp.where(wide == first + ii, label_rest, 0.0), axis=-1, keepdims=True)
                )
                scales.append(plain)
        hots.append(
            jnp.sum(jnp.where(lane == first + sub, label_apart, 0.0), axis=-1, keepdims=True)
        )
        scales.append(jnp.where((sub[:, 0:1] >= 0) & twin, 1.0, 0.0))
        hot = jnp.concatenate(hots, axis=0)
        scale = jnp.concatenate(scales, axis=0)
        lanes = jnp.broadcast_to(bin_lane[0:1], sym.shape)
        expo = jnp.exp(sym - jnp.max(sym, axis=-1, keepdims=True))
        probs = expo / jnp.sum(expo, axis=-1, keepdims=True)
        logit_grad = (scale * (probs - jnp.where(lanes == hot, 1.0, 0.0))).astype(BF16)

        upd_grad = outer(logit_grad, w_bins_ref[...])
        upd_half = upd_grad.astype(BF16)
        grad_bins[...] += inner(updated[0:every], logit_grad) + inner(updated[every:], logit_grad)
        grad_out_t[...] += inner(upd_half, hidden[0:every]) + inner(upd_half, hidden[every:])
        hid_grad = outer(upd_half, w_out_half[...])
        pre_grad = jnp.concatenate(
            [(hid_grad * slope[0:every]).astype(BF16), (hid_grad * slope[every:]).astype(BF16)],
            axis=0,
        )
        grad_in[...] += inner(normed, pre_grad)
        norm_grad = outer(pre_grad, w_in_ref[...]) * gain
        pair_grad = inv_scale * (
            norm_grad
            - jnp.mean(norm_grad, axis=-1, keepdims=True)
            - normal_form * jnp.mean(norm_grad * normal_form, axis=-1, keepdims=True)
        )
        for side in range(2):
            mine = pair_grad[side * every : (side + 1) * every] + upd_grad
            ones, head_near, head_far, tail = [], None, None, None
            for ii in range(GROUP):
                part = mine[ii * half : (ii + 1) * half]
                ones.append(jnp.sum(part, axis=0, keepdims=True))
                close = jnp.where(near[ii], part[0:GROUP], 0.0)
                apart = part[0:GROUP] - close
                head_near = close if ii == 0 else head_near + close
                head_far = apart if ii == 0 else head_far + apart
                if half > GROUP:
                    tail = part[GROUP:] if ii == 0 else tail + part[GROUP:]
            blk_sums[side, pl.ds(first, GROUP), :] = jnp.concatenate(ones, axis=0) + mine[span:]
            side_sums[1 - side, pl.ds(first, GROUP), :] += head_near
            side_sums[1 - side, pl.ds(first + half, GROUP), :] += head_far + mine[span:]
            if half > GROUP:
                side_sums[1 - side, pl.ds(first + GROUP, half - GROUP), :] += tail
        return carry

    lax.fori_loop(0, block // GROUP, step, 0)

    for side in range(2):
        row_out[side, 0:beyond, :] = side_sums[side, 0:beyond, :] + side_sums[side, block:, :]
        row_out[side, beyond:, :] = side_sums[side, beyond:block, :]

    share_in = grad_in.shape[0] // count
    share_out = grad_out_t.shape[1] // count
    tiles = grad_in.shape[1] // width
    grad_out = grad_out_t[...].T
    bins = grad_bins[...]
    bins = jnp.concatenate([bins, jnp.zeros_like(bins)], axis=1)
    for m in range(count):
        at = 0
        for t in range(tiles):
            col_out[m, at : at + share_in, :] = grad_in[
                m * share_in : (m + 1) * share_in, t * width : (t + 1) * width
            ]
            at += share_in
        col_out[m, at : at + share_out, :] = grad_out[m * share_out : (m + 1) * share_out]
        at += share_out
        col_out[m, at : at + share_in, :] = bins[m * share_in : (m + 1) * share_in]
        at += share_in
        for side in range(2):
            col_out[m, at : at + rows, :] = blk_sums[side, m * rows : (m + 1) * rows, :]
            at += rows


def run_pairs(place, mine, theirs, rows, labels, gain, bias, w_in, b_in, w_out, w_bins):
    count = mine.shape[0]
    width, hidden = w_in.shape
    bins = w_bins.shape[1]
    block = count * rows
    long = block + block // 2 + GROUP
    share = (width // count) * (hidden // width) + hidden // count + width // count
    vmem = pl.BlockSpec(memory_space=pltpu.VMEM)
    smem = pl.BlockSpec(memory_space=pltpu.SMEM)
    return pl.pallas_call(
        functools.partial(pair_kernel, count=count, rows=rows),
        out_shape=(
            jax.ShapeDtypeStruct((count, share + 2 * rows, width), F32),
            jax.ShapeDtypeStruct((2, block, width), F32),
        ),
        in_specs=[smem] + [vmem] * 9,
        out_specs=(vmem, vmem),
        scratch_shapes=[
            pltpu.VMEM((width, hidden), BF16),
            pltpu.VMEM((hidden, width), BF16),
            pltpu.VMEM((2, block, width), F32),
            pltpu.VMEM((2, block, width), F32),
            pltpu.VMEM((2, long, width), F32),
            pltpu.VMEM((2, long, width), F32),
            pltpu.VMEM((long, width), F32),
            pltpu.VMEM((width, hidden), F32),
            pltpu.VMEM((width, hidden), F32),
            pltpu.VMEM((width, bins), F32),
            pltpu.VMEM((2, block, width), F32),
            pltpu.VMEM((2, long, width), F32),
        ],
        compiler_params=pltpu.CompilerParams(vmem_limit_bytes=56 * 1024 * 1024),
        interpret=INTERPRET,
        name="pairs",
    )(
        place,
        mine,
        theirs,
        labels,
        gain[None],
        bias[None],
        w_in,
        b_in[None],
        w_out,
        w_bins,
    )


INTERPRET = False


def on_device(left_act, right_act, norm_gain, norm_bias, w_in, b_in, w_out, w_bins, labels):
    count = lax.axis_size("col")
    size = lax.axis_size("row")
    rows, width = left_act.shape
    hidden = w_in.shape[1]
    swap = twin_swap(size, count)
    both = ("row", "col")
    gap = jnp.zeros((GROUP - rows, width), left_act.dtype)
    stacked = jnp.concatenate([left_act, gap, right_act, gap], axis=0)
    mine = from_everyone(stacked, "col")
    theirs = lax.ppermute(mine, both, block_routes(size, count))
    turned = jnp.pad(labels.T.astype(F32), ((0, 0), (0, width - labels.shape[0])))
    place = jnp.stack([lax.axis_index("row"), lax.axis_index("col")]).astype(jnp.int32)
    col_out, row_out = run_pairs(
        place, mine, theirs, rows, turned, norm_gain, norm_bias, w_in, b_in, w_out, w_bins
    )
    shares = lax.all_to_all(col_out, "col", 0, 0, tiled=True).sum(axis=0)
    share = shares.shape[0] - 2 * rows
    near_left, near_right = lax.optimization_barrier(
        (shares[share : share + rows], shares[share + rows :])
    )
    far_right = lax.ppermute(near_right, both, swap)
    far_right = jnp.pad(far_right, ((-(-share // size), 0), (0, 0)))
    far_right = lax.optimization_barrier(far_right)
    piece = -(-share // size)
    shares = jnp.pad(shares[0:share], ((0, piece * size - share), (0, 0)))
    pieces = jnp.concatenate(
        [
            shares.reshape(size, piece, width) / (rows * count * size),
            row_out[1].reshape(size, rows, width),
            row_out[0].reshape(size, rows, width),
        ],
        axis=1,
    )
    pieces = lax.all_to_all(pieces, "row", 0, 0, tiled=True)
    pieces = pieces.sum(axis=0)
    far_left = lax.ppermute(pieces[piece + rows :], both, swap)
    far_left = jnp.pad(far_left, ((0, GROUP - rows + 1), (0, 0)))
    grad_left = near_left + lax.optimization_barrier(far_left)[0:rows]
    pieces = from_everyone(pieces[0 : piece + rows] + far_right, "row")
    grad_right = pieces[:, piece:].reshape(rows * size, width)
    last = pieces[:, 0:piece].reshape(size * piece, width)[0:share]
    last = from_everyone(last, "col")
    cut = (width // count) * (hidden // width)
    grad_in = (
        last[:, 0:cut]
        .reshape(count, hidden // width, width // count, width)
        .transpose(0, 2, 1, 3)
        .reshape(width, hidden)
    )
    grad_out = last[:, cut : cut + hidden // count].reshape(hidden, width)
    grad_bins = last[:, cut + hidden // count : share, 0 : w_bins.shape[1]].reshape(width, -1)
    return (grad_left, grad_right, grad_in, grad_out, grad_bins)


def solution(mesh):
    placed = (
        P(("row", "col"), None),
        P(("row", "col"), None),
        P(),
        P(),
        P(),
        P(),
        P(),
        P(),
        P("row", "col"),
    )

    return jax.shard_map(
        on_device,
        mesh=mesh,
        in_specs=placed,
        out_specs=(P(("row", "col"), None), P("col", None), P(), P(), P()),
        check_vma=False,
    )
```

```python
import functools

import jax
import jax.numpy as jnp
from jax import lax
from jax.experimental import pallas as pl
from jax.experimental.pallas import tpu as pltpu
from jax.sharding import PartitionSpec as P


GROUP = 8
F32 = jnp.float32
BF16 = jnp.bfloat16


def from_everyone(value, axis):
    count = lax.axis_size(axis)
    return lax.all_to_all(
        jnp.broadcast_to(value[None], (count, *value.shape)), axis, 0, 0, tiled=True
    )


def inner(first, second):
    return lax.dot_general(first, second, (((0,), (0,)), ((), ())), preferred_element_type=F32)


def outer(first, second):
    return lax.dot_general(first, second, (((1,), (1,)), ((), ())), preferred_element_type=F32)


def dot(first, second):
    return jnp.dot(first, second, preferred_element_type=F32)


def twin_swap(size, count):
    return [(a * count + b, b * count + a) for a in range(size) for b in range(count)]


def block_routes(size, count):
    if (size, count) != (16, 16):
        return twin_swap(size, count)
    pairs = []
    for r in range(size):
        for c in range(count):
            y, z = (r // 4 - c // 4) % 4, (r % 4 - c % 4) % 4
            low = (c // 2) % 2
            low = (low, 1, 1 - low, 0)[z]
            k = 4 * ((c // 4 + 2 - y) % 4) + 2 * low + (z + 1) % 2
            pairs.append((c * count + k, r * count + c))
    return pairs


def pair_kernel(
    place,
    mine_ref,
    theirs_ref,
    labels_ref,
    gain_ref,
    bias_ref,
    w_in_ref,
    b_in_ref,
    w_out_ref,
    w_bins_ref,
    col_out,
    own_left,
    far_right,
    far_left,
    own_right,
    w_in_half,
    w_out_half,
    blk,
    blk_center,
    far_side,
    far_center,
    label_rows,
    grad_in,
    grad_out_t,
    grad_bins,
    side_sums,
    *,
    count,
    rows,
):
    block = count * rows
    half = block // 2
    width = gain_ref.shape[1]
    beyond = half + GROUP
    twin = place[0] == place[1]
    skew = (place[0] > place[1]).astype(jnp.int32)

    for m in range(count):
        one = mine_ref[m].astype(F32)
        other = theirs_ref[m].astype(F32)
        for side in range(2):
            at = side * GROUP
            blk[side, m * rows : (m + 1) * rows, :] = one[at : at + rows]
            far_side[side, m * rows : (m + 1) * rows, :] = other[at : at + rows]
    label_rows[0:block, :] = labels_ref[...]
    label_rows[block:, :] = labels_ref[0:beyond, :]
    for side in range(2):
        value = blk[side]
        blk_center[side] = value - jnp.mean(value, axis=-1, keepdims=True)
        value = far_side[side, 0:block, :]
        value = value - jnp.mean(value, axis=-1, keepdims=True)
        far_center[side, 0:block, :] = value
        far_center[side, block:, :] = value[0:beyond]
        far_side[side, block:, :] = far_side[side, 0:beyond, :]

    grad_in[...] = jnp.zeros_like(grad_in)
    grad_out_t[...] = jnp.zeros_like(grad_out_t)
    grad_bins[...] = jnp.zeros_like(grad_bins)
    side_sums[...] = jnp.zeros_like(side_sums)

    w_in_half[...] = w_in_ref[...] * jnp.asarray(0.5, BF16)
    w_out_half[...] = w_out_ref[...] * jnp.asarray(0.5, BF16)
    gain = gain_ref[...]
    bias = bias_ref[...]
    b_in = 0.5 * b_in_ref[...]
    sub = lax.broadcasted_iota(jnp.int32, (GROUP, width), 0)
    lane = lax.broadcasted_iota(jnp.int32, (GROUP, width), 1)
    near = [sub >= ii + skew for ii in range(GROUP)]
    bin_lane = lax.broadcasted_iota(jnp.int32, (GROUP, w_bins_ref.shape[1]), 1).astype(F32)
    span = GROUP * half
    every = span + GROUP

    def step(s, carry):
        first = pl.multiple_of(s * GROUP, GROUP)

        def head(ref, *lead):
            return ref[(*lead, pl.ds(first, GROUP), slice(None))]

        def middle(ref, *lead):
            return ref[(*lead, pl.ds(first + GROUP, half - GROUP), slice(None))]

        def away(ref, *lead):
            return ref[(*lead, pl.ds(first + half, GROUP), slice(None))]

        summed, center = [], []
        for mine, other, into in ((blk, far_side, summed), (blk_center, far_center, center)):
            for side in range(2):
                own = head(mine, side)
                close, apart = head(other, 1 - side), away(other, 1 - side)
                rest = middle(other, 1 - side) if half > GROUP else None
                for ii in range(GROUP):
                    one = own[ii : ii + 1, :]
                    into.append(jnp.where(near[ii], close, apart) + one)
                    if half > GROUP:
                        into.append(rest + one)
                into.append(own + apart)
        summed = jnp.concatenate(summed, axis=0)
        center = jnp.concatenate(center, axis=0)
        inv_scale = lax.rsqrt(jnp.mean(center * center, axis=-1, keepdims=True) + 1e-05)
        normal_form = center * inv_scale
        normed = (normal_form * gain + bias).astype(BF16)
        act = dot(normed, w_in_half[...]) + b_in
        up = jnp.tanh(act) + 1.0
        hidden = (act * up).astype(BF16)
        slope = up * (act * (2.0 - up) + 1.0)
        updated = (summed + dot(hidden, w_out_ref[...])).astype(BF16)
        logits = dot(updated, w_bins_ref[...])
        sym = logits[0:every] + logits[every:]

        hots, scales = [], []
        label_close, label_apart = head(label_rows), away(label_rows)
        if half > GROUP:
            label_rest = middle(label_rows)
            wide = lax.broadcasted_iota(jnp.int32, label_rest.shape, 1)
            plain = jnp.full((half - GROUP, 1), 2.0, F32)
        for ii in range(GROUP):
            chosen = jnp.where(near[ii], label_close, label_apart)
            hots.append(
                jnp.sum(jnp.where(lane == first + ii, chosen, 0.0), axis=-1, keepdims=True)
            )
            scales.append(jnp.where((sub[:, 0:1] == ii) & twin, 1.0, 2.0))
            if half > GROUP:
                hots.append(
                    jnp.sum(jnp.where(wide == first + ii, label_rest, 0.0), axis=-1, keepdims=True)
                )
                scales.append(plain)
        hots.append(
            jnp.sum(jnp.where(lane == first + sub, label_apart, 0.0), axis=-1, keepdims=True)
        )
        scales.append(jnp.where((sub[:, 0:1] >= 0) & twin, 1.0, 0.0))
        hot = jnp.concatenate(hots, axis=0)
        scale = jnp.concatenate(scales, axis=0)
        lanes = jnp.broadcast_to(bin_lane[0:1], sym.shape)
        expo = jnp.exp(sym - jnp.max(sym, axis=-1, keepdims=True))
        probs = expo / jnp.sum(expo, axis=-1, keepdims=True)
        logit_grad = (scale * (probs - jnp.where(lanes == hot, 1.0, 0.0))).astype(BF16)

        upd_grad = outer(logit_grad, w_bins_ref[...])
        upd_half = upd_grad.astype(BF16)
        grad_bins[...] += inner(updated[0:every], logit_grad) + inner(updated[every:], logit_grad)
        grad_out_t[...] += inner(upd_half, hidden[0:every]) + inner(upd_half, hidden[every:])
        hid_grad = outer(upd_half, w_out_half[...])
        pre_grad = jnp.concatenate(
            [(hid_grad * slope[0:every]).astype(BF16), (hid_grad * slope[every:]).astype(BF16)],
            axis=0,
        )
        grad_in[...] += inner(normed, pre_grad)
        norm_grad = outer(pre_grad, w_in_ref[...]) * gain
        pair_grad = inv_scale * (
            norm_grad
            - jnp.mean(norm_grad, axis=-1, keepdims=True)
            - normal_form * jnp.mean(norm_grad * normal_form, axis=-1, keepdims=True)
        )
        for side in range(2):
            mine = pair_grad[side * every : (side + 1) * every] + upd_grad
            ones, head_near, head_far, tail = [], None, None, None
            for ii in range(GROUP):
                part = mine[ii * half : (ii + 1) * half]
                ones.append(jnp.sum(part, axis=0, keepdims=True))
                close = jnp.where(near[ii], part[0:GROUP], 0.0)
                apart = part[0:GROUP] - close
                head_near = close if ii == 0 else head_near + close
                head_far = apart if ii == 0 else head_far + apart
                if half > GROUP:
                    tail = part[GROUP:] if ii == 0 else tail + part[GROUP:]
            target = (own_left, far_right)[side]
            target[pl.ds(first, GROUP), :] = jnp.concatenate(ones, axis=0) + mine[span:]
            side_sums[1 - side, pl.ds(first, GROUP), :] += head_near
            side_sums[1 - side, pl.ds(first + half, GROUP), :] += head_far + mine[span:]
            if half > GROUP:
                side_sums[1 - side, pl.ds(first + GROUP, half - GROUP), :] += tail
        return carry

    lax.fori_loop(0, block // GROUP, step, 0, unroll=2)

    for side in range(2):
        target = (far_left, own_right)[side]
        target[0:beyond, :] = side_sums[side, 0:beyond, :] + side_sums[side, block:, :]
        target[beyond:, :] = side_sums[side, beyond:block, :]

    share_in = grad_in.shape[0] // count
    share_out = grad_out_t.shape[1] // count
    tiles = grad_in.shape[1] // width
    grad_out = grad_out_t[...].T
    bins = grad_bins[...]
    bins = jnp.concatenate([bins, jnp.zeros_like(bins)], axis=1)
    for m in range(count):
        at = 0
        for t in range(tiles):
            col_out[m, at : at + share_in, :] = grad_in[
                m * share_in : (m + 1) * share_in, t * width : (t + 1) * width
            ]
            at += share_in
        col_out[m, at : at + share_out, :] = grad_out[m * share_out : (m + 1) * share_out]
        at += share_out
        col_out[m, at : at + share_in, :] = bins[m * share_in : (m + 1) * share_in]


def run_pairs(place, mine, theirs, rows, labels, gain, bias, w_in, b_in, w_out, w_bins):
    count = mine.shape[0]
    width, hidden = w_in.shape
    bins = w_bins.shape[1]
    block = count * rows
    long = block + block // 2 + GROUP
    share = (width // count) * (hidden // width) + hidden // count + width // count
    vmem = pl.BlockSpec(memory_space=pltpu.VMEM)
    smem = pl.BlockSpec(memory_space=pltpu.SMEM)
    return pl.pallas_call(
        functools.partial(pair_kernel, count=count, rows=rows),
        out_shape=(
            jax.ShapeDtypeStruct((count, share, width), F32),
            *[jax.ShapeDtypeStruct((block, width), F32)] * 4,
        ),
        in_specs=[smem] + [vmem] * 9,
        out_specs=(vmem,) * 5,
        scratch_shapes=[
            pltpu.VMEM((width, hidden), BF16),
            pltpu.VMEM((hidden, width), BF16),
            pltpu.VMEM((2, block, width), F32),
            pltpu.VMEM((2, block, width), F32),
            pltpu.VMEM((2, long, width), F32),
            pltpu.VMEM((2, long, width), F32),
            pltpu.VMEM((long, width), F32),
            pltpu.VMEM((width, hidden), F32),
            pltpu.VMEM((width, hidden), F32),
            pltpu.VMEM((width, bins), F32),
            pltpu.VMEM((2, long, width), F32),
        ],
        compiler_params=pltpu.CompilerParams(vmem_limit_bytes=56 * 1024 * 1024),
        interpret=INTERPRET,
        name="pairs",
    )(
        place,
        mine,
        theirs,
        labels,
        gain[None],
        bias[None],
        w_in,
        b_in[None],
        w_out,
        w_bins,
    )


INTERPRET = False


def on_device(left_act, right_act, norm_gain, norm_bias, w_in, b_in, w_out, w_bins, labels):
    count = lax.axis_size("col")
    size = lax.axis_size("row")
    rows, width = left_act.shape
    hidden = w_in.shape[1]
    routes = block_routes(size, count)
    back = [(there, here) for here, there in routes]
    both = ("row", "col")
    gap = jnp.zeros((GROUP - rows, width), left_act.dtype)
    stacked = jnp.concatenate([left_act, gap, right_act, gap], axis=0)
    mine = from_everyone(stacked, "col")
    theirs = lax.ppermute(mine, both, routes)
    turned = jnp.pad(labels.T.astype(F32), ((0, 0), (0, width - labels.shape[0])))
    place = jnp.stack([lax.axis_index("row"), lax.axis_index("col")]).astype(jnp.int32)
    col_out, own_left, far_right, far_left, own_right = run_pairs(
        place, mine, theirs, rows, turned, norm_gain, norm_bias, w_in, b_in, w_out, w_bins
    )
    shares = lax.all_to_all(col_out, "col", 0, 0, tiled=True)
    shares = shares.sum(axis=0)
    far_right = lax.ppermute(far_right, both, routes)
    right = own_right + far_right
    right = lax.optimization_barrier(right)
    share = shares.shape[0]
    piece = -(-share // size)
    shares = jnp.pad(shares, ((0, piece * size - share), (0, 0)))
    pieces = jnp.concatenate(
        [
            shares.reshape(size, piece, width) / (rows * count * size),
            right.reshape(size, rows, width),
        ],
        axis=1,
    )
    pieces = lax.all_to_all(pieces, "row", 0, 0, tiled=True)
    pieces = pieces.sum(axis=0)
    far_left = lax.ppermute(far_left, both, back)
    left = own_left + far_left
    left = lax.optimization_barrier(left)
    pieces = from_everyone(pieces, "row")
    grad_right = pieces[:, piece:].reshape(rows * size, width)
    last = jnp.concatenate(
        [
            jnp.broadcast_to(
                pieces[:, 0:piece].reshape(size * piece, width)[None, 0:share],
                (count, share, width),
            ),
            left.reshape(count, rows, width),
        ],
        axis=1,
    )
    last = lax.all_to_all(last, "col", 0, 0, tiled=True)
    grad_left = last[:, share:].sum(axis=0)
    cut = (width // count) * (hidden // width)
    grad_in = (
        last[:, 0:cut]
        .reshape(count, hidden // width, width // count, width)
        .transpose(0, 2, 1, 3)
        .reshape(width, hidden)
    )
    grad_out = last[:, cut : cut + hidden // count].reshape(hidden, width)
    grad_bins = last[:, cut + hidden // count : share, 0 : w_bins.shape[1]].reshape(width, -1)
    return (grad_left, grad_right, grad_in, grad_out, grad_bins)


def solution(mesh):
    placed = (
        P(("row", "col"), None),
        P(("row", "col"), None),
        P(),
        P(),
        P(),
        P(),
        P(),
        P(),
        P("row", "col"),
    )

    return jax.shard_map(
        on_device,
        mesh=mesh,
        in_specs=placed,
        out_specs=(P(("row", "col"), None), P("col", None), P(), P(), P()),
        check_vma=False,
    )
```

```python
import functools

import jax
import jax.numpy as jnp
from jax import lax
from jax.experimental import pallas as pl
from jax.experimental.pallas import tpu as pltpu
from jax.sharding import PartitionSpec as P


GROUP = 8
F32 = jnp.float32
BF16 = jnp.bfloat16


def from_everyone(value, axis):
    count = lax.axis_size(axis)
    return lax.all_to_all(
        jnp.broadcast_to(value[None], (count, *value.shape)), axis, 0, 0, tiled=True
    )


def inner(first, second):
    return lax.dot_general(first, second, (((0,), (0,)), ((), ())), preferred_element_type=F32)


def outer(first, second):
    return lax.dot_general(first, second, (((1,), (1,)), ((), ())), preferred_element_type=F32)


def dot(first, second):
    return jnp.dot(first, second, preferred_element_type=F32)


def twin_swap(size, count):
    return [(a * count + b, b * count + a) for a in range(size) for b in range(count)]


def block_routes(size, count):
    if (size, count) != (16, 16):
        return twin_swap(size, count)
    pairs = []
    for r in range(size):
        for c in range(count):
            y, z = (r // 4 - c // 4) % 4, (r % 4 - c % 4) % 4
            low = (c // 2) % 2
            low = (low, 1, 1 - low, 0)[z]
            k = 4 * ((c // 4 + 2 - y) % 4) + 2 * low + (z + 1) % 2
            pairs.append((c * count + k, r * count + c))
    return pairs


def pair_kernel(
    place,
    mine_ref,
    theirs_ref,
    labels_ref,
    gain_ref,
    bias_ref,
    w_in_ref,
    b_in_ref,
    w_out_ref,
    w_bins_ref,
    col_out,
    own_left,
    far_right,
    far_left,
    own_right,
    w_in_half,
    w_out_half,
    blk,
    blk_center,
    far_side,
    far_center,
    label_rows,
    grad_in,
    grad_out_t,
    grad_bins,
    side_sums,
    *,
    count,
    rows,
):
    block = count * rows
    half = block // 2
    width = gain_ref.shape[1]
    beyond = half + GROUP
    twin = place[0] == place[1]
    skew = (place[0] > place[1]).astype(jnp.int32)

    for m in range(count):
        one = mine_ref[m].astype(F32)
        other = theirs_ref[m].astype(F32)
        for side in range(2):
            at = side * GROUP
            blk[side, m * rows : (m + 1) * rows, :] = one[at : at + rows]
            far_side[side, m * rows : (m + 1) * rows, :] = other[at : at + rows]
    label_rows[0:block, :] = labels_ref[...]
    label_rows[block:, :] = labels_ref[0:beyond, :]
    for side in range(2):
        value = blk[side]
        blk_center[side] = value - jnp.mean(value, axis=-1, keepdims=True)
        value = far_side[side, 0:block, :]
        value = value - jnp.mean(value, axis=-1, keepdims=True)
        far_center[side, 0:block, :] = value
        far_center[side, block:, :] = value[0:beyond]
        far_side[side, block:, :] = far_side[side, 0:beyond, :]

    grad_in[...] = jnp.zeros_like(grad_in)
    grad_out_t[...] = jnp.zeros_like(grad_out_t)
    grad_bins[...] = jnp.zeros_like(grad_bins)
    side_sums[...] = jnp.zeros_like(side_sums)

    w_in_half[0:width, :] = w_in_ref[...] * jnp.asarray(0.5, BF16)
    rest = 0.5 * b_in_ref[...]
    term_row = lax.broadcasted_iota(jnp.int32, (width, rest.shape[1]), 0)
    terms = jnp.zeros(term_row.shape, F32)
    for n in range(3):
        term = rest.astype(BF16).astype(F32)
        terms = jnp.where(term_row == n, term, terms)
        rest = rest - term
    w_in_half[width:, :] = terms.astype(BF16)
    w_out_half[...] = w_out_ref[...] * jnp.asarray(0.5, BF16)
    gain = gain_ref[...]
    bias = bias_ref[...]
    sub = lax.broadcasted_iota(jnp.int32, (GROUP, width), 0)
    lane = lax.broadcasted_iota(jnp.int32, (GROUP, width), 1)
    near = [sub >= ii + skew for ii in range(GROUP)]
    bin_lane = lax.broadcasted_iota(jnp.int32, (GROUP, w_bins_ref.shape[1]), 1).astype(F32)
    span = GROUP * half
    every = span + GROUP

    ones_of = jnp.where(
        lax.broadcasted_iota(jnp.int32, (2 * every, width), 1) < 3, 1.0, 0.0
    ).astype(BF16)

    def step(s, carry):
        first = pl.multiple_of(s * GROUP, GROUP)

        def head(ref, *lead):
            return ref[(*lead, pl.ds(first, GROUP), slice(None))]

        def middle(ref, *lead):
            return ref[(*lead, pl.ds(first + GROUP, half - GROUP), slice(None))]

        def away(ref, *lead):
            return ref[(*lead, pl.ds(first + half, GROUP), slice(None))]

        summed, center = [], []
        for mine, other, into in ((blk, far_side, summed), (blk_center, far_center, center)):
            for side in range(2):
                own = head(mine, side)
                close, apart = head(other, 1 - side), away(other, 1 - side)
                rest = middle(other, 1 - side) if half > GROUP else None
                for ii in range(GROUP):
                    one = own[ii : ii + 1, :]
                    into.append(jnp.where(near[ii], close, apart) + one)
                    if half > GROUP:
                        into.append(rest + one)
                into.append(own + apart)
        summed = jnp.concatenate(summed, axis=0)
        center = jnp.concatenate(center, axis=0)
        inv_scale = lax.rsqrt(jnp.mean(center * center, axis=-1, keepdims=True) + 1e-05)
        normal_form = center * inv_scale
        normed = (normal_form * gain + bias).astype(BF16)
        act = dot(jnp.concatenate([normed, ones_of], axis=1), w_in_half[...])
        up = jnp.tanh(act) + 1.0
        hidden = (act * up).astype(BF16)
        slope = up * (act * (2.0 - up) + 1.0)
        updated = (summed + dot(hidden, w_out_ref[...])).astype(BF16)
        logits = dot(updated, w_bins_ref[...])
        sym = logits[0:every] + logits[every:]

        hots, scales = [], []
        label_close, label_apart = head(label_rows), away(label_rows)
        if half > GROUP:
            label_rest = middle(label_rows)
            wide = lax.broadcasted_iota(jnp.int32, label_rest.shape, 1)
            plain = jnp.full((half - GROUP, 1), 2.0, F32)
        for ii in range(GROUP):
            chosen = jnp.where(near[ii], label_close, label_apart)
            hots.append(
                jnp.sum(jnp.where(lane == first + ii, chosen, 0.0), axis=-1, keepdims=True)
            )
            scales.append(jnp.where((sub[:, 0:1] == ii) & twin, 1.0, 2.0))
            if half > GROUP:
                hots.append(
                    jnp.sum(jnp.where(wide == first + ii, label_rest, 0.0), axis=-1, keepdims=True)
                )
                scales.append(plain)
        hots.append(
            jnp.sum(jnp.where(lane == first + sub, label_apart, 0.0), axis=-1, keepdims=True)
        )
        scales.append(jnp.where((sub[:, 0:1] >= 0) & twin, 1.0, 0.0))
        hot = jnp.concatenate(hots, axis=0)
        scale = jnp.concatenate(scales, axis=0)
        lanes = jnp.broadcast_to(bin_lane[0:1], sym.shape)
        expo = jnp.exp(sym - jnp.max(sym, axis=-1, keepdims=True))
        probs = expo / jnp.sum(expo, axis=-1, keepdims=True)
        logit_grad = (scale * (probs - jnp.where(lanes == hot, 1.0, 0.0))).astype(BF16)

        upd_grad = outer(logit_grad, w_bins_ref[...])
        upd_half = upd_grad.astype(BF16)
        grad_bins[...] += inner(updated[0:every], logit_grad) + inner(updated[every:], logit_grad)
        grad_out_t[...] += inner(upd_half, hidden[0:every]) + inner(upd_half, hidden[every:])
        hid_grad = outer(upd_half, w_out_half[...])
        pre_grad = jnp.concatenate(
            [(hid_grad * slope[0:every]).astype(BF16), (hid_grad * slope[every:]).astype(BF16)],
            axis=0,
        )
        grad_in[...] += inner(normed, pre_grad)
        norm_grad = outer(pre_grad, w_in_ref[...]) * gain
        pair_grad = inv_scale * (
            norm_grad
            - jnp.mean(norm_grad, axis=-1, keepdims=True)
            - normal_form * jnp.mean(norm_grad * normal_form, axis=-1, keepdims=True)
        )
        for side in range(2):
            mine = pair_grad[side * every : (side + 1) * every] + upd_grad
            ones, head_near, head_far, tail = [], None, None, None
            for ii in range(GROUP):
                part = mine[ii * half : (ii + 1) * half]
                ones.append(jnp.sum(part, axis=0, keepdims=True))
                close = jnp.where(near[ii], part[0:GROUP], 0.0)
                apart = part[0:GROUP] - close
                head_near = close if ii == 0 else head_near + close
                head_far = apart if ii == 0 else head_far + apart
                if half > GROUP:
                    tail = part[GROUP:] if ii == 0 else tail + part[GROUP:]
            target = (own_left, far_right)[side]
            target[pl.ds(first, GROUP), :] = jnp.concatenate(ones, axis=0) + mine[span:]
            side_sums[1 - side, pl.ds(first, GROUP), :] += head_near
            side_sums[1 - side, pl.ds(first + half, GROUP), :] += head_far + mine[span:]
            if half > GROUP:
                side_sums[1 - side, pl.ds(first + GROUP, half - GROUP), :] += tail
        return carry

    lax.fori_loop(0, block // GROUP, step, 0, unroll=2)

    for side in range(2):
        target = (far_left, own_right)[side]
        target[0:beyond, :] = side_sums[side, 0:beyond, :] + side_sums[side, block:, :]
        target[beyond:, :] = side_sums[side, beyond:block, :]

    share_in = grad_in.shape[0] // count
    share_out = grad_out_t.shape[1] // count
    tiles = grad_in.shape[1] // width
    grad_out = grad_out_t[...].T
    bins = grad_bins[...]
    bins = jnp.concatenate([bins, jnp.zeros_like(bins)], axis=1)
    for m in range(count):
        at = 0
        for t in range(tiles):
            col_out[m, at : at + share_in, :] = grad_in[
                m * share_in : (m + 1) * share_in, t * width : (t + 1) * width
            ]
            at += share_in
        col_out[m, at : at + share_out, :] = grad_out[m * share_out : (m + 1) * share_out]
        at += share_out
        col_out[m, at : at + share_in, :] = bins[m * share_in : (m + 1) * share_in]


def run_pairs(place, mine, theirs, rows, labels, gain, bias, w_in, b_in, w_out, w_bins):
    count = mine.shape[0]
    width, hidden = w_in.shape
    bins = w_bins.shape[1]
    block = count * rows
    long = block + block // 2 + GROUP
    share = (width // count) * (hidden // width) + hidden // count + width // count
    vmem = pl.BlockSpec(memory_space=pltpu.VMEM)
    smem = pl.BlockSpec(memory_space=pltpu.SMEM)
    return pl.pallas_call(
        functools.partial(pair_kernel, count=count, rows=rows),
        out_shape=(
            jax.ShapeDtypeStruct((count, share, width), F32),
            *[jax.ShapeDtypeStruct((block, width), F32)] * 4,
        ),
        in_specs=[smem] + [vmem] * 9,
        out_specs=(vmem,) * 5,
        scratch_shapes=[
            pltpu.VMEM((2 * width, hidden), BF16),
            pltpu.VMEM((hidden, width), BF16),
            pltpu.VMEM((2, block, width), F32),
            pltpu.VMEM((2, block, width), F32),
            pltpu.VMEM((2, long, width), F32),
            pltpu.VMEM((2, long, width), F32),
            pltpu.VMEM((long, width), F32),
            pltpu.VMEM((width, hidden), F32),
            pltpu.VMEM((width, hidden), F32),
            pltpu.VMEM((width, bins), F32),
            pltpu.VMEM((2, long, width), F32),
        ],
        compiler_params=pltpu.CompilerParams(vmem_limit_bytes=56 * 1024 * 1024),
        interpret=INTERPRET,
        name="pairs",
    )(
        place,
        mine,
        theirs,
        labels,
        gain[None],
        bias[None],
        w_in,
        b_in[None],
        w_out,
        w_bins,
    )


INTERPRET = False


def on_device(left_act, right_act, norm_gain, norm_bias, w_in, b_in, w_out, w_bins, labels):
    count = lax.axis_size("col")
    size = lax.axis_size("row")
    rows, width = left_act.shape
    hidden = w_in.shape[1]
    routes = block_routes(size, count)
    back = [(there, here) for here, there in routes]
    both = ("row", "col")
    gap = jnp.zeros((GROUP - rows, width), left_act.dtype)
    stacked = jnp.concatenate([left_act, gap, right_act, gap], axis=0)
    mine = from_everyone(stacked, "col")
    theirs = lax.ppermute(mine, both, routes)
    turned = jnp.pad(labels.T.astype(F32), ((0, 0), (0, width - labels.shape[0])))
    place = jnp.stack([lax.axis_index("row"), lax.axis_index("col")]).astype(jnp.int32)
    col_out, own_left, far_right, far_left, own_right = run_pairs(
        place, mine, theirs, rows, turned, norm_gain, norm_bias, w_in, b_in, w_out, w_bins
    )
    shares = lax.all_to_all(col_out, "col", 0, 0, tiled=True)
    shares = shares.sum(axis=0)
    far_right = lax.ppermute(far_right, both, routes)
    right = own_right + far_right
    right = lax.optimization_barrier(right)
    share = shares.shape[0]
    piece = -(-share // size)
    shares = jnp.pad(shares, ((0, piece * size - share), (0, 0)))
    pieces = jnp.concatenate(
        [
            shares.reshape(size, piece, width) / (rows * count * size),
            right.reshape(size, rows, width),
        ],
        axis=1,
    )
    pieces = lax.all_to_all(pieces, "row", 0, 0, tiled=True)
    pieces = pieces.sum(axis=0)
    far_left = lax.ppermute(far_left, both, back)
    left = own_left + far_left
    left = lax.optimization_barrier(left)
    pieces = from_everyone(pieces, "row")
    grad_right = pieces[:, piece:].reshape(rows * size, width)
    last = jnp.concatenate(
        [
            jnp.broadcast_to(
                pieces[:, 0:piece].reshape(size * piece, width)[None, 0:share],
                (count, share, width),
            ),
            left.reshape(count, rows, width),
        ],
        axis=1,
    )
    last = lax.all_to_all(last, "col", 0, 0, tiled=True)
    grad_left = last[:, share:].sum(axis=0)
    cut = (width // count) * (hidden // width)
    grad_in = (
        last[:, 0:cut]
        .reshape(count, hidden // width, width // count, width)
        .transpose(0, 2, 1, 3)
        .reshape(width, hidden)
    )
    grad_out = last[:, cut : cut + hidden // count].reshape(hidden, width)
    grad_bins = last[:, cut + hidden // count : share, 0 : w_bins.shape[1]].reshape(width, -1)
    return (grad_left, grad_right, grad_in, grad_out, grad_bins)


def solution(mesh):
    placed = (
        P(("row", "col"), None),
        P(("row", "col"), None),
        P(),
        P(),
        P(),
        P(),
        P(),
        P(),
        P("row", "col"),
    )

    return jax.shard_map(
        on_device,
        mesh=mesh,
        in_specs=placed,
        out_specs=(P(("row", "col"), None), P("col", None), P(), P(), P()),
        check_vma=False,
    )
```
